32 devices in a mesh: gx: 4 (over z), gz: 4 (over y, x), gy: 2 (over core).
Axes of the slice: x: 2, y: 2, z: 4, core: 2. Of those that a mesh axis runs over, the one named last changes fastest.
Arguments:
- row_embed: bfloat16 [65536, 128], P(('gx', 'gz')), may hold values from -24 to 24, as said below
- col_embed: bfloat16 [1024, 128], P('gy'), may hold values from -24 to 24, as said below
- row_mass: float32 [65536], P(('gx', 'gz')), may hold values from 1 to 10
- col_mass: float32 [1024], P('gy'), may hold values from 1 to 10
Outputs:
- row_potential: float32 [65536], P(('gx', 'gz'))
- col_potential: float32 [1024], P('gy')
- errors: float32 [10, 2], replicated
The draws below stay inside these ranges and needn't reach their ends.
Inputs may be any that keep to these rules, and one draw needn't show every extreme that they name: `row_embed`: entries are real-valued embedding coordinates. `col_embed`: entries are real-valued embedding coordinates.
All inputs are finite; a program needn't handle non-finite values.
Results may differ from the reference program's by a relative error of at most 0.0003.
Values sent between devices are 32-bit elements; how exact they have to be, the bound alone decides.
A program may use at most 64 MiB of HBM per device.

```python
import math
import jax
import jax.numpy as jnp
from jax import lax

E = 128
ITERS = 10
NR = 65536
NC = 1024


def embed_draw(key, count):
    base = jnp.clip(jax.random.normal(jax.random.fold_in(key, 11), (count, E), jnp.float32), -6.0, 6.0)
    return base.astype(jnp.bfloat16)


def draw_row_embed(key, part):
    return embed_draw(jax.random.fold_in(key, 1), NR)


def draw_col_embed(key, part):
    return embed_draw(jax.random.fold_in(key, 2), NC)


def block_levels(rng, dims, cuts, smallest, top_value):
    gain, own = 1.0, jax.random.fold_in(rng, 6)
    for dim, parts in cuts:
        steps = jnp.exp(jax.random.uniform(jax.random.fold_in(own, dim), (parts,), jnp.float32, smallest / len(cuts), top_value / len(cuts)))
        gain = gain * jnp.repeat(steps, dims[dim] // parts).reshape([-1 if axis == dim else 1 for axis in range(len(dims))])
    return gain


def setup_inputs(seed: int = 0) -> dict:
    seeds = jax.random.split(jax.random.key(seed), 5)
    return {
        "row_embed": draw_row_embed(jax.random.fold_in(seeds[4], 71), 0),
        "col_embed": draw_col_embed(jax.random.fold_in(seeds[4], 71), 0),
        "row_mass": jnp.clip(jnp.exp(math.log(10.0) - 2.3025851 * jax.random.uniform(seeds[2], (NR,), jnp.float32) ** block_levels(seeds[2], (NR,), ((0, 16),), -0.2, 0.2)), 1.0, 10.0),
        "col_mass": jnp.clip(jnp.exp(math.log(10.0) - 2.3025851 * jax.random.uniform(seeds[3], (NC,), jnp.float32) ** block_levels(seeds[3], (NC,), ((0, 2),), -0.2, 0.2)), 1.0, 10.0),
    }


eps = 0.05


def cost_block(xb, col_embed, col_sq):
    cross = jnp.dot(xb, col_embed.T, preferred_element_type=jnp.float32)
    xf = xb.astype(jnp.float32)
    row_sq = jnp.sum(xf * xf, axis=1)
    return (row_sq[:, None] + col_sq[None, :] - 2.0 * cross) / E


def reference(row_embed, col_embed, row_mass, col_mass):
    mass_a = row_mass / jnp.sum(row_mass)
    mass_b = col_mass / jnp.sum(col_mass)
    log_a = jnp.log(mass_a)
    log_b = jnp.log(mass_b)
    yf = col_embed.astype(jnp.float32)
    col_sq = jnp.sum(yf * yf, axis=1)
    block = math.gcd(NR, 2048)
    count = NR // block
    xblocks = row_embed.reshape(count, block, E)

    def row_lse(g_pot):
        def one(xb):
            z = (g_pot[None, :] - cost_block(xb, col_embed, col_sq)) / eps
            top = jnp.max(z, axis=1)
            return top + jnp.log(jnp.sum(jnp.exp(z - top[:, None]), axis=1))
        return lax.map(one, xblocks).reshape(NR)

    def col_lse(f_pot):
        fblocks = f_pot.reshape(count, block)

        def step(carry, item):
            top, total = carry
            xb, fb = item
            z = (fb[:, None] - cost_block(xb, col_embed, col_sq)) / eps
            newtop = jnp.maximum(top, jnp.max(z, axis=0))
            total = total * jnp.exp(top - newtop) + jnp.sum(jnp.exp(z - newtop[None, :]), axis=0)
            return (newtop, total), None
        start = (jnp.full((NC,), -jnp.inf, jnp.float32), jnp.zeros((NC,), jnp.float32))
        (top, total), unused = lax.scan(step, start, (xblocks, fblocks))
        return top + jnp.log(total)

    f_pot = jnp.zeros((NR,), jnp.float32)
    g_pot = jnp.zeros((NC,), jnp.float32)
    rows_out = []
    for index in range(ITERS):
        f_new = eps * (log_a - row_lse(g_pot))
        rows_out.append(jnp.sum(jnp.abs(jnp.exp(log_a + (f_pot - f_new) / eps) - mass_a)))
        f_pot = f_new
        g_new = eps * (log_b - col_lse(f_pot))
        rows_out.append(jnp.sum(jnp.abs(jnp.exp(log_b + (g_pot - g_new) / eps) - mass_b)))
        g_pot = g_new
    errors = jnp.stack(rows_out).reshape(ITERS, 2)
    return f_pot, g_pot, errors
```

```python
import functools
import math

import jax
import jax.numpy as jnp
from jax import lax
from jax.experimental import pallas as pl
from jax.experimental.pallas import tpu as pltpu
from jax.sharding import PartitionSpec as P

ITERS = 10
eps = 0.05
LANES = 128
CHUNK = 8
SUB = 32
SCALE = math.log2(math.e) / eps
F32 = jnp.float32
MESH = pl.DeviceIdType.MESH


def kernel(nx, nz, ny, x_hbm, y_hbm, rm_hbm, cm_hbm, f_out, g_out, e_out,
           m_ref, t_ref, f_ref, r_ref, a_ref, rho_ref, cap_ref, gc_ref, b_ref,
           err0_ref, errs_ref, w_ref, v_ref, lse_ref, rbuf0, rbuf, cbuf0, cbuf, ebuf,
           x_ref, y_ref, rm_ref, cm_ref, s_x, s_y, s_m, s_r0, r_r0, s_r, r_r, s_c0, r_c0, s_c, r_c, s_e, r_e):
    rows, width = x_ref.shape
    cols = y_ref.shape[0]
    tiles = rows // LANES
    ctiles = cols // LANES
    chunks = tiles // CHUNK
    nsub = cols // SUB
    gb, ga, gl, gu = range(tiles, tiles + 4)
    ix, iz, iy = lax.axis_index("gx"), lax.axis_index("gz"), lax.axis_index("gy")
    ng = nx * nz
    me = ix * nz + iz
    pad = ebuf.shape[1]

    def col_peer(d):
        other = lax.rem(me + d, ng)
        return {"gx": other // nz, "gz": lax.rem(other, nz)}

    def row_peer(d):
        return {"gy": lax.rem(iy + d, ny)}

    barrier = pltpu.get_barrier_semaphore()
    for d in range(1, ng):
        pl.semaphore_signal(barrier, inc=1, device_id=col_peer(d), device_id_type=MESH)
    for d in range(1, ny):
        pl.semaphore_signal(barrier, inc=1, device_id=row_peer(d), device_id_type=MESH)

    y_copy = pltpu.make_async_copy(y_hbm, y_ref, s_y)
    y_copy.start()
    half = rows // 2
    x_copies = [pltpu.make_async_copy(x_hbm.at[pl.ds(h * half, half)], x_ref.at[pl.ds(h * half, half)], s_x.at[h])
                for h in range(2)]
    m_copies = [pltpu.make_async_copy(cm_hbm, cm_ref, s_m.at[0]), pltpu.make_async_copy(rm_hbm, rm_ref, s_m.at[1])]
    for copy in x_copies + m_copies:
        copy.start()

    def send(buf, ssem, rsem, peers):
        for peer in peers:
            pltpu.make_async_remote_copy(
                src_ref=buf, dst_ref=buf, send_sem=ssem, recv_sem=rsem,
                device_id=peer, device_id_type=MESH).start()

    def drain(some, sem):
        pltpu.make_async_copy(some, some, sem).wait()

    def flip(p, bit):
        return p + bit - 2 * bit * lax.rem(p // bit, 2)

    def far_peer(i):
        px, pz = ix, iz
        for step in range(ng.bit_length()):
            bit = 1 << step
            if (i // nz) & bit:
                px = flip(px, bit)
            if (i % nz) & bit:
                pz = flip(pz, bit)
        return {"gx": px, "gz": pz}

    if nx & (nx - 1) or nz & (nz - 1):
        col_peers = [col_peer(d) for d in range(1, ng)]
    else:
        col_peers = [far_peer(i) for i in range(ng - 1, 0, -1)]
    row_peers = [row_peer(d) for d in range(1, ny)]

    def spread(compact, slot):
        for t in range(ctiles):
            block = jnp.broadcast_to(compact[t:t + 1, :], (LANES, LANES))
            t_ref[slot, t * LANES:(t + 1) * LANES, :] = jnp.transpose(block)

    def squeeze(op):
        return jnp.concatenate(
            [op(jnp.transpose(t_ref[ga, t * LANES:(t + 1) * LANES, :]), axis=0, keepdims=True)
             for t in range(ctiles)], axis=0)

    factor = 2.0 * SCALE / width
    ones = jnp.ones((8, width), jnp.bfloat16)
    nt = (((1,), (1,)), ((), ()))
    group = math.gcd(CHUNK, 4)

    def fold(v, op):
        out = v[0:8]
        for q in range(1, v.shape[0] // 8):
            out = op(out, v[q * 8:(q + 1) * 8])
        return out

    def row_norm(v):
        square = v * v
        high = square.astype(jnp.bfloat16)
        low = (square - high.astype(F32)).astype(jnp.bfloat16)
        parts = [lax.dot_general(ones, part, nt, preferred_element_type=F32) for part in (high, low)]
        return (parts[0] + parts[1]) * (SCALE / width)

    y_copy.wait()
    yv = y_ref[...]
    yf = yv.astype(F32)
    ysq = row_norm(yf)
    kap = jnp.concatenate([ysq[0:1, t * LANES:(t + 1) * LANES] for t in range(ctiles)], axis=0)
    cap_ref[...] = kap
    spread(-kap, gb)
    for copy in m_copies:
        copy.wait()
    csum = jnp.broadcast_to(jnp.sum(cm_ref[...], axis=0, keepdims=True), (CHUNK, LANES))
    for c in range(chunks):
        rbuf0[c, iy, 2 * CHUNK:3 * CHUNK, :] = csum

    def build(i, carry):
        xb = x_ref[pl.ds(pl.multiple_of(i * group * LANES, group * LANES), group * LANES), :]
        prod = lax.dot_general(y_ref[...], xb, nt, preferred_element_type=F32) * factor
        for q in range(group):
            m_ref[i * group + q] = prod[:, q * LANES:(q + 1) * LANES]
        tops = [None] * group
        for s in range(nsub):
            sl = slice(s * SUB, (s + 1) * SUB)
            gv = t_ref[gb, sl, :]
            for q in range(group):
                part = fold(m_ref[i * group + q, sl, :] + gv, jnp.maximum)
                tops[q] = part if tops[q] is None else jnp.maximum(tops[q], part)
        tops = [jnp.max(top, axis=0, keepdims=True) for top in tops]
        tots = [jnp.zeros((8, LANES), F32) for q in range(group)]
        for s in range(nsub):
            sl = slice(s * SUB, (s + 1) * SUB)
            gv = t_ref[gb, sl, :]
            for q in range(group):
                val = jnp.exp2((m_ref[i * group + q, sl, :] + gv) - tops[q])
                tots[q] = tots[q] + fold(val, jnp.add)
        c = i * group // CHUNK
        for q in range(group):
            at = lax.rem(i * group, CHUNK) + q
            rbuf0[c, iy, pl.ds(at, 1), :] = tops[q]
            rbuf0[c, iy, pl.ds(CHUNK + at, 1), :] = jnp.sum(tots[q], axis=0, keepdims=True)
        return carry

    steps = tiles // group
    x_copies[0].wait()
    lax.fori_loop(0, steps // 2, build, 0)
    x_copies[1].wait()
    lax.fori_loop(steps // 2, steps, build, 0)
    pl.semaphore_wait(barrier, (ng - 1) + (ny - 1))

    def push0(c, carry):
        send(rbuf0.at[c, iy], s_r0.at[c], r_r0.at[c], row_peers)
        return carry

    lax.fori_loop(0, chunks, push0, 0)
    t_ref[ga] = jnp.full((cols, LANES), -jnp.inf, F32)

    def colmax(c, carry):
        drain(rbuf0.at[c, 0:ny - 1], r_r0.at[c])
        drain(rbuf0.at[c, 0:ny - 1], s_r0.at[c])
        top = rbuf0[c, 0, 0:CHUNK, :]
        for d in range(1, ny):
            top = jnp.maximum(top, rbuf0[c, d, 0:CHUNK, :])
        tot = jnp.zeros((CHUNK, LANES), F32)
        for d in range(ny):
            tot = tot + rbuf0[c, d, CHUNK:2 * CHUNK, :] * jnp.exp2(rbuf0[c, d, 0:CHUNK, :] - top)
        lse = top + jnp.log2(tot)
        sl8 = pl.ds(pl.multiple_of(c * CHUNK, CHUNK), CHUNK)
        lse_ref[sl8, :] = lse
        fv = jnp.log2(rm_ref[sl8, :]) - lse
        f_ref[sl8, :] = fv
        w_ref[...] = fv
        for s in range(nsub):
            sl = slice(s * SUB, (s + 1) * SUB)
            acc = t_ref[ga, sl, :]
            for q in range(CHUNK):
                acc = jnp.maximum(acc, m_ref[c * CHUNK + q, sl, :] + w_ref[q:q + 1, :])
            t_ref[ga, sl, :] = acc
        return carry

    lax.fori_loop(0, chunks, colmax, 0)
    ctop = squeeze(jnp.max)
    spread(ctop, gb)
    t_ref[ga] = jnp.zeros((cols, LANES), F32)

    def colsum(c, carry):
        w_ref[...] = f_ref[pl.ds(pl.multiple_of(c * CHUNK, CHUNK), CHUNK), :]
        for s in range(nsub):
            sl = slice(s * SUB, (s + 1) * SUB)
            acc = t_ref[ga, sl, :]
            gv = t_ref[gb, sl, :]
            for q in range(CHUNK):
                val = jnp.exp2((m_ref[c * CHUNK + q, sl, :] + w_ref[q:q + 1, :]) - gv)
                t_ref[c * CHUNK + q, sl, :] = val
                acc = acc + val
            t_ref[ga, sl, :] = acc
        return carry

    lax.fori_loop(0, chunks, colsum, 0)
    ctot = rbuf0[0, 0, 2 * CHUNK:2 * CHUNK + 1, :]
    for d in range(1, ny):
        ctot = ctot + rbuf0[0, d, 2 * CHUNK:2 * CHUNK + 1, :]
    mass = rm_ref[...]
    cbuf0[me, 0:ctiles, :] = ctop
    cbuf0[me, ctiles:2 * ctiles, :] = squeeze(jnp.sum)
    cbuf0[me, 2 * ctiles:2 * ctiles + 1, :] = jnp.sum(mass, axis=0, keepdims=True)
    send(cbuf0.at[me], s_c0, r_c0, col_peers)
    b_ref[...] = cm_ref[...] / jnp.sum(ctot, axis=1, keepdims=True)

    def norms(i, carry):
        xf = x_ref[pl.ds(pl.multiple_of(i * group * LANES, group * LANES), group * LANES), :].astype(F32)
        sq = row_norm(xf)
        for q in range(group):
            rho_ref[pl.ds(i * group + q, 1), :] = sq[0:1, q * LANES:(q + 1) * LANES]
        return carry

    lax.fori_loop(0, tiles // group, norms, 0)
    errs_ref[...] = jnp.zeros_like(errs_ref)
    ebuf[iy] = jnp.zeros(ebuf.shape[1:], F32)
    drain(cbuf0.at[0:ng - 1], r_c0)
    top = cbuf0[0, 0:ctiles, :]
    rtot = cbuf0[0, 2 * ctiles:2 * ctiles + 1, :]
    for d in range(1, ng):
        top = jnp.maximum(top, cbuf0[d, 0:ctiles, :])
        rtot = rtot + cbuf0[d, 2 * ctiles:2 * ctiles + 1, :]
    tot = jnp.zeros((ctiles, LANES), F32)
    for d in range(ng):
        tot = tot + cbuf0[d, ctiles:2 * ctiles, :] * jnp.exp2(cbuf0[d, 0:ctiles, :] - top)
    bv = b_ref[...]
    v_ref[...] = bv * jnp.exp2(cbuf0[me, 0:ctiles, :] - top) / tot
    rtot = jnp.sum(rtot, axis=1, keepdims=True)
    lrt = jnp.log2(rtot)
    a = rm_ref[...] / rtot
    a_ref[...] = a
    f_ref[...] = f_ref[...] - lrt
    err0_ref[...] = jnp.sum(jnp.abs(jnp.exp2(lse_ref[...] - rho_ref[...]) - a), axis=0, keepdims=True)
    clse = top + jnp.log2(tot) - lrt
    gc_ref[...] = jnp.log2(bv) - clse
    ebuf[iy, 0:1, :] = jnp.sum(jnp.abs(jnp.exp2(clse - cap_ref[...]) - bv), axis=0, keepdims=True)
    drain(cbuf0.at[0:ng - 1], s_c0)

    def rebuild(i, carry):
        fvs = [f_ref[pl.ds(i * group + q, 1), :] for q in range(group)]
        for s in range(nsub):
            sl = slice(s * SUB, (s + 1) * SUB)
            gv = t_ref[gl, sl, :]
            for q in range(group):
                t_ref[i * group + q, sl, :] = jnp.exp2((m_ref[i * group + q, sl, :] + gv) + fvs[q])
        return carry

    def iteration(k, carry):
        par = lax.rem(k, 2)
        spread(v_ref[...], gb)
        for c in range(chunks):
            tots = [None] * CHUNK
            for s in range(nsub):
                sl = slice(s * SUB, (s + 1) * SUB)
                gv = t_ref[gb, sl, :]
                for q in range(CHUNK):
                    part = fold(t_ref[c * CHUNK + q, sl, :] * gv, jnp.add)
                    tots[q] = part if tots[q] is None else tots[q] + part
            for q in range(CHUNK):
                rbuf[par, c, iy, q:q + 1, :] = jnp.sum(tots[q], axis=0, keepdims=True)
            send(rbuf.at[par, c, iy], s_r.at[par, c], r_r.at[par, c], row_peers)
        per = LANES // SUB
        for c in range(chunks):
            drain(rbuf.at[par, c, 0:ny - 1], r_r.at[par, c])
            r = rbuf[par, c, 0]
            for d in range(1, ny):
                r = r + rbuf[par, c, d]
            sl8 = slice(c * CHUNK, (c + 1) * CHUNK)
            r_ref[sl8, :] = r
            t_ref[gu, sl8, :] = a_ref[sl8, :] / r
            for t in range(ctiles):
                block = []
                for s in range(t * per, (t + 1) * per):
                    sl = slice(s * SUB, (s + 1) * SUB)
                    acc = t_ref[ga, sl, :] if c else None
                    for q in range(c * CHUNK, (c + 1) * CHUNK):
                        val = t_ref[q, sl, :] * t_ref[gu, q:q + 1, :]
                        acc = val if acc is None else acc + val
                    if c < chunks - 1:
                        t_ref[ga, sl, :] = acc
                    block.append(acc)
                if c == chunks - 1:
                    line = jnp.sum(jnp.transpose(jnp.concatenate(block, axis=0)), axis=0, keepdims=True)
                    cbuf[par, me, t:t + 1, :] = line * v_ref[t:t + 1, :]
        cbuf[par, me, ctiles:ctiles + 1, :] = jnp.sum(jnp.abs(r_ref[...] - a_ref[...]), axis=0, keepdims=True)
        cbuf[par, me, ctiles + 1:ctiles + 2, :] = err0_ref[...]
        send(cbuf.at[par, me, 0:ctiles + 2], s_c.at[par], r_c.at[par], col_peers)
        f_ref[...] = f_ref[...] + jnp.log2(t_ref[gu, 0:tiles, :])
        spread(gc_ref[...], gl)
        lax.fori_loop(0, tiles // group, rebuild, 0)
        for c in range(chunks):
            drain(rbuf.at[par, c, 0:ny - 1], s_r.at[par, c])
        drain(cbuf.at[par, 0:ng - 1, 0:ctiles + 2], r_c.at[par])
        got = cbuf[par, 0]
        for d in range(1, ng):
            got = got + cbuf[par, d]
        old = got[0:ctiles]
        bv = b_ref[...]
        v = bv / old
        v_ref[...] = v
        gc_ref[...] = gc_ref[...] + jnp.log2(v)
        ebuf[iy, pl.ds(k, 1), :] = jnp.sum(jnp.abs(old - bv), axis=0, keepdims=True)
        errs_ref[pl.ds(k, 1), :] = got[ctiles:ctiles + 1]
        errs_ref[0:1, :] = got[ctiles + 1:ctiles + 2]
        drain(cbuf.at[par, 0:ng - 1, 0:ctiles + 2], s_c.at[par])
        return carry

    lax.fori_loop(1, ITERS, iteration, 0)
    send(ebuf.at[iy], s_e, r_e, row_peers)
    f_out[...] = (f_ref[...] + rho_ref[...]) * (1.0 / SCALE)
    g_out[...] = (gc_ref[...] + cap_ref[...]) * (1.0 / SCALE)
    drain(ebuf.at[0:ny - 1], r_e)
    drain(ebuf.at[0:ny - 1], s_e)
    ce = ebuf[0]
    for d in range(1, ny):
        ce = ce + ebuf[d]
    errs_ref[pad:2 * pad, :] = ce
    both = jnp.sum(jnp.transpose(errs_ref[...]), axis=0, keepdims=True)
    e_out[0:1, :] = both[:, 0:ITERS]
    e_out[1:2, :] = both[:, pad:pad + ITERS]


def on_device(row_embed, col_embed, row_mass, col_mass):
    rows, width = row_embed.shape
    cols = col_embed.shape[0]
    nx, nz, ny = lax.axis_size("gx"), lax.axis_size("gz"), lax.axis_size("gy")
    ng = nx * nz
    tiles, ctiles = rows // LANES, cols // LANES
    chunks = tiles // CHUNK
    pad = -(-ITERS // 8) * 8
    crow0 = -(-(2 * ctiles + 1) // 8) * 8
    crow = -(-(ctiles + 2) // 8) * 8
    vm = lambda *s: pltpu.VMEM(s, F32)
    dma = pltpu.SemaphoreType.DMA
    f, g, e = pl.pallas_call(
        functools.partial(kernel, nx, nz, ny),
        out_shape=(jax.ShapeDtypeStruct((tiles, LANES), F32),
                   jax.ShapeDtypeStruct((ctiles, LANES), F32),
                   jax.ShapeDtypeStruct((2, ITERS), F32)),
        in_specs=[pl.BlockSpec(memory_space=pl.ANY)] * 4,
        out_specs=[pl.BlockSpec(memory_space=pltpu.VMEM)] * 3,
        scratch_shapes=[
            vm(tiles, cols, LANES), vm(tiles + 4, cols, LANES),
            vm(tiles, LANES), vm(tiles, LANES), vm(tiles, LANES), vm(tiles, LANES),
            vm(ctiles, LANES), vm(ctiles, LANES), vm(ctiles, LANES),
            vm(1, LANES), vm(LANES, LANES), vm(CHUNK, LANES), vm(ctiles, LANES),
            vm(tiles, LANES), vm(chunks, ny, 3 * CHUNK, LANES), vm(2, chunks, ny, CHUNK, LANES),
            vm(ng, crow0, LANES), vm(2, ng, crow, LANES), vm(ny, pad, LANES),
            pltpu.VMEM((rows, width), row_embed.dtype), pltpu.VMEM((cols, width), col_embed.dtype),
            vm(tiles, LANES), vm(ctiles, LANES), dma((2,)), dma, dma((2,)), dma((chunks,)), dma((chunks,)), dma((2, chunks)), dma((2, chunks)), dma, dma, dma((2,)), dma((2,)), dma, dma,
        ],
        compiler_params=pltpu.CompilerParams(
            collective_id=0, has_side_effects=True, vmem_limit_bytes=67043328),
    )(row_embed, col_embed, row_mass.reshape(tiles, LANES), col_mass.reshape(ctiles, LANES))
    return f.reshape(rows), g.reshape(cols), e.T


def solution(mesh):
    in_specs = (P(("gx", "gz"), None), P("gy", None), P(("gx", "gz")), P("gy"))
    out_specs = (P(("gx", "gz")), P("gy"), P())
    return jax.shard_map(
        on_device, mesh=mesh, in_specs=in_specs, out_specs=out_specs, check_vma=False
    )
```

```python
import functools
import math

import jax
import jax.numpy as jnp
from jax import lax
from jax.experimental import pallas as pl
from jax.experimental.pallas import tpu as pltpu
from jax.sharding import PartitionSpec as P

ITERS = 10
eps = 0.05
LANES = 128
CHUNK = 8
SUB = 32
SCALE = math.log2(math.e) / eps
F32 = jnp.float32
MESH = pl.DeviceIdType.MESH


def kernel(nx, nz, ny, x_hbm, y_hbm, rm_hbm, cm_hbm, f_out, g_out, e_out,
           m_ref, t_ref, f_ref, r_ref, a_ref, rho_ref, cap_ref, gc_ref, b_ref,
           err0_ref, errs_ref, w_ref, v_ref, lse_ref, rbuf0, rbuf, cbuf0, cbuf, ebuf,
           x_ref, y_ref, rm_ref, cm_ref, s_x, s_y, s_m, s_r0, r_r0, s_r, r_r, s_c0, r_c0, s_c, r_c, s_e, r_e):
    rows, width = x_ref.shape
    cols = y_ref.shape[0]
    tiles = rows // LANES
    ctiles = cols // LANES
    chunks = tiles // CHUNK
    nsub = cols // SUB
    gb, ga, gl, gu = range(tiles, tiles + 4)
    ix, iz, iy = lax.axis_index("gx"), lax.axis_index("gz"), lax.axis_index("gy")
    ng = nx * nz
    me = ix * nz + iz
    pad = ebuf.shape[1]

    def col_peer(d):
        other = lax.rem(me + d, ng)
        return {"gx": other // nz, "gz": lax.rem(other, nz)}

    def row_peer(d):
        return {"gy": lax.rem(iy + d, ny)}

    y_copy = pltpu.make_async_copy(y_hbm, y_ref, s_y)
    y_copy.start()
    first = tiles // CHUNK // 2 * CHUNK * LANES
    cuts = (slice(0, first), slice(first, rows))
    x_copies = [pltpu.make_async_copy(x_hbm.at[cut], x_ref.at[cut], s_x.at[h]) for h, cut in enumerate(cuts)]
    m_copies = [pltpu.make_async_copy(cm_hbm, cm_ref, s_m.at[0]), pltpu.make_async_copy(rm_hbm, rm_ref, s_m.at[1])]
    for copy in x_copies + m_copies:
        copy.start()

    barrier = pltpu.get_barrier_semaphore()
    for d in range(1, ng):
        pl.semaphore_signal(barrier, inc=1, device_id=col_peer(d), device_id_type=MESH)
    for d in range(1, ny):
        pl.semaphore_signal(barrier, inc=1, device_id=row_peer(d), device_id_type=MESH)

    def send(buf, ssem, rsem, peers):
        for peer in peers:
            pltpu.make_async_remote_copy(
                src_ref=buf, dst_ref=buf, send_sem=ssem, recv_sem=rsem,
                device_id=peer, device_id_type=MESH).start()

    def drain(some, sem):
        pltpu.make_async_copy(some, some, sem).wait()

    def flip(p, bit):
        return p + bit - 2 * bit * lax.rem(p // bit, 2)

    def far_peer(i):
        px, pz = ix, iz
        for step in range(ng.bit_length()):
            bit = 1 << step
            if (i // nz) & bit:
                px = flip(px, bit)
            if (i % nz) & bit:
                pz = flip(pz, bit)
        return {"gx": px, "gz": pz}

    if nx & (nx - 1) or nz & (nz - 1):
        col_peers = [col_peer(d) for d in range(1, ng)]
    else:
        col_peers = [far_peer(i) for i in range(ng - 1, 0, -1)]
    row_peers = [row_peer(d) for d in range(1, ny)]

    def spread(compact, slot):
        for t in range(ctiles):
            block = jnp.broadcast_to(compact[t:t + 1, :], (LANES, LANES))
            t_ref[slot, t * LANES:(t + 1) * LANES, :] = jnp.transpose(block)

    def squeeze(op):
        return jnp.concatenate(
            [op(jnp.transpose(t_ref[ga, t * LANES:(t + 1) * LANES, :]), axis=0, keepdims=True)
             for t in range(ctiles)], axis=0)

    factor = 2.0 * SCALE / width
    ones = jnp.ones((8, width), jnp.bfloat16)
    nt = (((1,), (1,)), ((), ()))
    group = math.gcd(CHUNK, 4)

    def fold(v, op):
        out = v[0:8]
        for q in range(1, v.shape[0] // 8):
            out = op(out, v[q * 8:(q + 1) * 8])
        return out

    def row_norm(v):
        square = v * v
        high = square.astype(jnp.bfloat16)
        low = (square - high.astype(F32)).astype(jnp.bfloat16)
        parts = [lax.dot_general(ones, part, nt, preferred_element_type=F32) for part in (high, low)]
        return (parts[0] + parts[1]) * (SCALE / width)

    y_copy.wait()
    yv = y_ref[...]
    yf = yv.astype(F32)
    ysq = row_norm(yf)
    kap = jnp.concatenate([ysq[0:1, t * LANES:(t + 1) * LANES] for t in range(ctiles)], axis=0)
    cap_ref[...] = kap
    spread(-kap, gb)
    for copy in m_copies:
        copy.wait()
    csum = jnp.broadcast_to(jnp.sum(cm_ref[...], axis=0, keepdims=True), (CHUNK, LANES))
    for c in range(chunks):
        rbuf0[c, iy, 2 * CHUNK:3 * CHUNK, :] = csum

    def product(i):
        xb = x_ref[i * group * LANES:(i + 1) * group * LANES, :]
        prod = lax.dot_general(y_ref[...], xb, nt, preferred_element_type=F32)
        tops = [None] * group
        for s in range(nsub):
            sl = slice(s * SUB, (s + 1) * SUB)
            gv = t_ref[gb, sl, :]
            for q in range(group):
                val = prod[sl, q * LANES:(q + 1) * LANES] * factor + gv
                m_ref[i * group + q, sl, :] = val
                part = fold(val, jnp.maximum)
                tops[q] = part if tops[q] is None else jnp.maximum(tops[q], part)
        return [jnp.max(top, axis=0, keepdims=True) for top in tops]

    def row_sums(i, tops):
        tots = [None] * group
        for s in range(nsub):
            sl = slice(s * SUB, (s + 1) * SUB)
            for q in range(group):
                part = fold(jnp.exp2(m_ref[i * group + q, sl, :] - tops[q]), jnp.add)
                tots[q] = part if tots[q] is None else tots[q] + part
        c, at = divmod(i * group, CHUNK)
        for q in range(group):
            rbuf0[c, iy, at + q:at + q + 1, :] = tops[q]
            rbuf0[c, iy, CHUNK + at + q:CHUNK + at + q + 1, :] = jnp.sum(tots[q], axis=0, keepdims=True)

    steps = tiles // group
    per = CHUNK // group
    half = chunks // 2 * per
    x_copies[0].wait()
    tops = product(0)
    for i in range(steps):
        if i + 1 == half:
            x_copies[1].wait()
        ahead = product(i + 1) if i + 1 < steps else None
        row_sums(i, tops)
        tops = ahead
        if i + 1 == half:
            pl.semaphore_wait(barrier, (ng - 1) + (ny - 1))
            for c in range(half // per):
                send(rbuf0.at[c, iy], s_r0.at[c], r_r0.at[c], row_peers)
        elif i + 1 > half and (i + 1) % per == 0:
            c = i // per
            send(rbuf0.at[c, iy], s_r0.at[c], r_r0.at[c], row_peers)
    for c in range(chunks):
        drain(rbuf0.at[c, 0:ny - 1], r_r0.at[c])
        top = rbuf0[c, 0, 0:CHUNK, :]
        for d in range(1, ny):
            top = jnp.maximum(top, rbuf0[c, d, 0:CHUNK, :])
        tot = jnp.zeros((CHUNK, LANES), F32)
        for d in range(ny):
            tot = tot + rbuf0[c, d, CHUNK:2 * CHUNK, :] * jnp.exp2(rbuf0[c, d, 0:CHUNK, :] - top)
        lse = top + jnp.log2(tot)
        sl8 = slice(c * CHUNK, (c + 1) * CHUNK)
        lse_ref[sl8, :] = lse
        fv = jnp.log2(rm_ref[sl8, :]) - lse
        f_ref[sl8, :] = fv
        t_ref[gu, sl8, :] = fv
        for s in range(nsub):
            sl = slice(s * SUB, (s + 1) * SUB)
            acc = t_ref[ga, sl, :] if c else None
            for q in range(c * CHUNK, (c + 1) * CHUNK):
                val = m_ref[q, sl, :] + t_ref[gu, q:q + 1, :]
                acc = val if acc is None else jnp.maximum(acc, val)
            t_ref[ga, sl, :] = acc
    for c in range(chunks):
        drain(rbuf0.at[c, 0:ny - 1], s_r0.at[c])
    ctop = squeeze(jnp.max)
    spread(ctop, gb)
    for c in range(chunks):
        for s in range(nsub):
            sl = slice(s * SUB, (s + 1) * SUB)
            acc = t_ref[ga, sl, :] if c else None
            gv = t_ref[gb, sl, :]
            for q in range(c * CHUNK, (c + 1) * CHUNK):
                val = jnp.exp2((m_ref[q, sl, :] + t_ref[gu, q:q + 1, :]) - gv)
                t_ref[q, sl, :] = val
                acc = val if acc is None else acc + val
            t_ref[ga, sl, :] = acc
    ctot = rbuf0[0, 0, 2 * CHUNK:2 * CHUNK + 1, :]
    for d in range(1, ny):
        ctot = ctot + rbuf0[0, d, 2 * CHUNK:2 * CHUNK + 1, :]
    mass = rm_ref[...]
    cbuf0[me, 0:ctiles, :] = ctop
    cbuf0[me, ctiles:2 * ctiles, :] = squeeze(jnp.sum)
    cbuf0[me, 2 * ctiles:2 * ctiles + 1, :] = jnp.sum(mass, axis=0, keepdims=True)
    send(cbuf0.at[me], s_c0, r_c0, col_peers)
    b_ref[...] = cm_ref[...] / jnp.sum(ctot, axis=1, keepdims=True)

    def norms(i, carry):
        xf = x_ref[pl.ds(pl.multiple_of(i * group * LANES, group * LANES), group * LANES), :].astype(F32)
        sq = row_norm(xf)
        for q in range(group):
            rho_ref[pl.ds(i * group + q, 1), :] = sq[0:1, q * LANES:(q + 1) * LANES]
        return carry

    lax.fori_loop(0, tiles // group, norms, 0)
    errs_ref[...] = jnp.zeros_like(errs_ref)
    ebuf[iy] = jnp.zeros(ebuf.shape[1:], F32)
    drain(cbuf0.at[0:ng - 1], r_c0)
    top = cbuf0[0, 0:ctiles, :]
    rtot = cbuf0[0, 2 * ctiles:2 * ctiles + 1, :]
    for d in range(1, ng):
        top = jnp.maximum(top, cbuf0[d, 0:ctiles, :])
        rtot = rtot + cbuf0[d, 2 * ctiles:2 * ctiles + 1, :]
    tot = jnp.zeros((ctiles, LANES), F32)
    for d in range(ng):
        tot = tot + cbuf0[d, ctiles:2 * ctiles, :] * jnp.exp2(cbuf0[d, 0:ctiles, :] - top)
    bv = b_ref[...]
    v_ref[...] = bv * jnp.exp2(cbuf0[me, 0:ctiles, :] - top) / tot
    rtot = jnp.sum(rtot, axis=1, keepdims=True)
    lrt = jnp.log2(rtot)
    a = rm_ref[...] / rtot
    a_ref[...] = a
    f_ref[...] = f_ref[...] - lrt
    err0_ref[...] = jnp.sum(jnp.abs(jnp.exp2(lse_ref[...] - rho_ref[...]) - a), axis=0, keepdims=True)
    clse = top + jnp.log2(tot) - lrt
    kap = cap_ref[...]
    gc_ref[...] = jnp.log2(bv) - clse - kap
    ebuf[iy, 0:1, :] = jnp.sum(jnp.abs(jnp.exp2(clse) - bv), axis=0, keepdims=True)
    drain(cbuf0.at[0:ng - 1], s_c0)

    def rebuild(i, carry):
        fvs = [f_ref[pl.ds(i * group + q, 1), :] for q in range(group)]
        for s in range(nsub):
            sl = slice(s * SUB, (s + 1) * SUB)
            gv = t_ref[gl, sl, :]
            for q in range(group):
                t_ref[i * group + q, sl, :] = jnp.exp2((m_ref[i * group + q, sl, :] + gv) + fvs[q])
        return carry

    def iteration(k, carry):
        par = lax.rem(k, 2)
        spread(v_ref[...], gb)
        for c in range(chunks):
            tots = [None] * CHUNK
            for s in range(nsub):
                sl = slice(s * SUB, (s + 1) * SUB)
                gv = t_ref[gb, sl, :]
                for q in range(CHUNK):
                    part = fold(t_ref[c * CHUNK + q, sl, :] * gv, jnp.add)
                    tots[q] = part if tots[q] is None else tots[q] + part
            for q in range(CHUNK):
                rbuf[par, c, iy, q:q + 1, :] = jnp.sum(tots[q], axis=0, keepdims=True)
            send(rbuf.at[par, c, iy], s_r.at[par, c], r_r.at[par, c], row_peers)
        subs = LANES // SUB
        for c in range(chunks):
            drain(rbuf.at[par, c, 0:ny - 1], r_r.at[par, c])
            r = rbuf[par, c, 0]
            for d in range(1, ny):
                r = r + rbuf[par, c, d]
            sl8 = slice(c * CHUNK, (c + 1) * CHUNK)
            r_ref[sl8, :] = r
            t_ref[gu, sl8, :] = a_ref[sl8, :] / r
            for t in range(ctiles):
                block = []
                for s in range(t * subs, (t + 1) * subs):
                    sl = slice(s * SUB, (s + 1) * SUB)
                    acc = t_ref[ga, sl, :] if c else None
                    for q in range(c * CHUNK, (c + 1) * CHUNK):
                        val = t_ref[q, sl, :] * t_ref[gu, q:q + 1, :]
                        acc = val if acc is None else acc + val
                    if c < chunks - 1:
                        t_ref[ga, sl, :] = acc
                    block.append(acc)
                if c == chunks - 1:
                    line = jnp.sum(jnp.transpose(jnp.concatenate(block, axis=0)), axis=0, keepdims=True)
                    cbuf[par, me, t:t + 1, :] = line * v_ref[t:t + 1, :]
        cbuf[par, me, ctiles:ctiles + 1, :] = jnp.sum(jnp.abs(r_ref[...] - a_ref[...]), axis=0, keepdims=True)
        cbuf[par, me, ctiles + 1:ctiles + 2, :] = err0_ref[...]
        send(cbuf.at[par, me, 0:ctiles + 2], s_c.at[par], r_c.at[par], col_peers)
        f_ref[...] = f_ref[...] + jnp.log2(t_ref[gu, 0:tiles, :])
        spread(gc_ref[...] + cap_ref[...], gl)
        lax.fori_loop(0, tiles // group, rebuild, 0)
        for c in range(chunks):
            drain(rbuf.at[par, c, 0:ny - 1], s_r.at[par, c])
        drain(cbuf.at[par, 0:ng - 1, 0:ctiles + 2], r_c.at[par])
        got = cbuf[par, 0]
        for d in range(1, ng):
            got = got + cbuf[par, d]
        old = got[0:ctiles]
        bv = b_ref[...]
        v = bv / old
        v_ref[...] = v
        gc_ref[...] = gc_ref[...] + jnp.log2(v)
        ebuf[iy, pl.ds(k, 1), :] = jnp.sum(jnp.abs(old - bv), axis=0, keepdims=True)
        errs_ref[pl.ds(k, 1), :] = got[ctiles:ctiles + 1]
        errs_ref[0:1, :] = got[ctiles + 1:ctiles + 2]
        drain(cbuf.at[par, 0:ng - 1, 0:ctiles + 2], s_c.at[par])
        return carry

    lax.fori_loop(1, ITERS, iteration, 0)
    send(ebuf.at[iy], s_e, r_e, row_peers)
    f_out[...] = (f_ref[...] + rho_ref[...]) * (1.0 / SCALE)
    g_out[...] = (gc_ref[...] + cap_ref[...]) * (1.0 / SCALE)
    drain(ebuf.at[0:ny - 1], r_e)
    drain(ebuf.at[0:ny - 1], s_e)
    ce = ebuf[0]
    for d in range(1, ny):
        ce = ce + ebuf[d]
    errs_ref[pad:2 * pad, :] = ce
    both = jnp.sum(jnp.transpose(errs_ref[...]), axis=0, keepdims=True)
    e_out[0:1, :] = both[:, 0:ITERS]
    e_out[1:2, :] = both[:, pad:pad + ITERS]


def hand_on(f, g, e, f_out, g_out, e_out, sem):
    copies = [pltpu.make_async_copy(src, dst, sem.at[n])
              for n, (src, dst) in enumerate(((f, f_out), (g, g_out), (e, e_out)))]
    for copy in copies:
        copy.start()
    for copy in copies:
        copy.wait()


def on_device(row_embed, col_embed, row_mass, col_mass):
    rows, width = row_embed.shape
    cols = col_embed.shape[0]
    nx, nz, ny = lax.axis_size("gx"), lax.axis_size("gz"), lax.axis_size("gy")
    ng = nx * nz
    tiles, ctiles = rows // LANES, cols // LANES
    chunks = tiles // CHUNK
    pad = -(-ITERS // 8) * 8
    crow0 = -(-(2 * ctiles + 1) // 8) * 8
    crow = -(-(ctiles + 2) // 8) * 8
    vm = lambda *s: pltpu.VMEM(s, F32)
    dma = pltpu.SemaphoreType.DMA
    f, g, e = pl.pallas_call(
        functools.partial(kernel, nx, nz, ny),
        out_shape=(jax.ShapeDtypeStruct((tiles, LANES), F32),
                   jax.ShapeDtypeStruct((ctiles, LANES), F32),
                   jax.ShapeDtypeStruct((2, ITERS), F32)),
        in_specs=[pl.BlockSpec(memory_space=pl.ANY)] * 4,
        out_specs=[pl.BlockSpec(memory_space=pltpu.VMEM)] * 3,
        scratch_shapes=[
            vm(tiles, cols, LANES), vm(tiles + 4, cols, LANES),
            vm(tiles, LANES), vm(tiles, LANES), vm(tiles, LANES), vm(tiles, LANES),
            vm(ctiles, LANES), vm(ctiles, LANES), vm(ctiles, LANES),
            vm(1, LANES), vm(LANES, LANES), vm(CHUNK, LANES), vm(ctiles, LANES),
            vm(tiles, LANES), vm(chunks, ny, 3 * CHUNK, LANES), vm(2, chunks, ny, CHUNK, LANES),
            vm(ng, crow0, LANES), vm(2, ng, crow, LANES), vm(ny, pad, LANES),
            pltpu.VMEM((rows, width), row_embed.dtype), pltpu.VMEM((cols, width), col_embed.dtype),
            vm(tiles, LANES), vm(ctiles, LANES), dma((2,)), dma, dma((2,)), dma((chunks,)), dma((chunks,)), dma((2, chunks)), dma((2, chunks)), dma, dma, dma((2,)), dma((2,)), dma, dma,
        ],
        compiler_params=pltpu.CompilerParams(
            collective_id=0, has_side_effects=True, vmem_limit_bytes=67043328),
    )(row_embed, col_embed, row_mass.reshape(tiles, LANES), col_mass.reshape(ctiles, LANES))
    f, g, e = pl.pallas_call(
        hand_on,
        out_shape=tuple(jax.ShapeDtypeStruct(v.shape, F32) for v in (f, g, e)),
        in_specs=[pl.BlockSpec(memory_space=pl.ANY)] * 3,
        out_specs=[pl.BlockSpec(memory_space=pl.ANY)] * 3,
        scratch_shapes=[dma((3,))],
    )(f, g, e)
    return f.reshape(rows), g.reshape(cols), e.T


def solution(mesh):
    in_specs = (P(("gx", "gz"), None), P("gy", None), P(("gx", "gz")), P("gy"))
    out_specs = (P(("gx", "gz")), P("gy"), P())
    return jax.shard_map(
        on_device, mesh=mesh, in_specs=in_specs, out_specs=out_specs, check_vma=False
    )
```

```python
import functools
import math

import jax
import jax.numpy as jnp
from jax import lax
from jax.experimental import pallas as pl
from jax.experimental.pallas import tpu as pltpu
from jax.sharding import PartitionSpec as P

ITERS = 10
eps = 0.05
LANES = 128
CHUNK = 8
SUB = 32
SCALE = math.log2(math.e) / eps
F32 = jnp.float32
MESH = pl.DeviceIdType.MESH


def row_pieces(tiles):
    cuts = list(range(0, tiles, CHUNK // 2)) + [tiles]
    return list(zip(cuts[:-1], cuts[1:]))


def kernel(nx, nz, ny, x_hbm, y_hbm, rm_hbm, cm_hbm, f_out, g_out, e_out,
           m_ref, t_ref, f_ref, r_ref, a_ref, rho_ref, cap_ref, gc_ref, b_ref,
           err0_ref, le_ref, errs_ref, w_ref, v_ref, lse_ref, rbuf0, rbuf, cbuf0, cbuf, ebuf, obuf,
           x_ref, y_ref, rm_ref, cm_ref, s_x, s_y, s_m, s_r0, r_r0, s_r, r_r, s_c0, r_c0, s_c, r_c, s_e, r_e, s_o, r_o):
    rows, width = x_ref.shape
    cols = y_ref.shape[0]
    tiles = rows // LANES
    ctiles = cols // LANES
    chunks = tiles // CHUNK
    nsub = cols // SUB
    gb, ga, gl, gu = range(tiles, tiles + 4)
    pieces = row_pieces(tiles)
    ix, iz, iy = lax.axis_index("gx"), lax.axis_index("gz"), lax.axis_index("gy")
    ng = nx * nz
    me = ix * nz + iz
    pad = ebuf.shape[1]

    def col_peer(d):
        other = lax.rem(me + d, ng)
        return {"gx": other // nz, "gz": lax.rem(other, nz)}

    def row_peer(d):
        return {"gy": lax.rem(iy + d, ny)}

    y_copy = pltpu.make_async_copy(y_hbm, y_ref, s_y)
    y_copy.start()
    first = tiles // CHUNK // 2 * CHUNK * LANES
    cuts = (slice(0, first), slice(first, rows))
    x_copies = [pltpu.make_async_copy(x_hbm.at[cut], x_ref.at[cut], s_x.at[h]) for h, cut in enumerate(cuts)]
    m_copies = [pltpu.make_async_copy(cm_hbm, cm_ref, s_m.at[0]), pltpu.make_async_copy(rm_hbm, rm_ref, s_m.at[1])]
    for copy in x_copies + m_copies:
        copy.start()

    barrier = pltpu.get_barrier_semaphore()
    for d in range(1, ng):
        pl.semaphore_signal(barrier, inc=1, device_id=col_peer(d), device_id_type=MESH)
    for d in range(1, ny):
        for j in range(ng):
            peer = {**(col_peer(j) if j else {"gx": ix, "gz": iz}), **row_peer(d)}
            pl.semaphore_signal(barrier, inc=1, device_id=peer, device_id_type=MESH)

    def send(buf, ssem, rsem, peers):
        for peer in peers:
            pltpu.make_async_remote_copy(
                src_ref=buf, dst_ref=buf, send_sem=ssem, recv_sem=rsem,
                device_id=peer, device_id_type=MESH).start()

    def drain(some, sem):
        pltpu.make_async_copy(some, some, sem).wait()

    def flip(p, bit):
        return p + bit - 2 * bit * lax.rem(p // bit, 2)

    def far_peer(i):
        px, pz = ix, iz
        for step in range(ng.bit_length()):
            bit = 1 << step
            if (i // nz) & bit:
                px = flip(px, bit)
            if (i % nz) & bit:
                pz = flip(pz, bit)
        return {"gx": px, "gz": pz}

    if nx & (nx - 1) or nz & (nz - 1):
        col_peers = [col_peer(d) for d in range(1, ng)]
    else:
        col_peers = [far_peer(i) for i in range(ng - 1, 0, -1)]
    row_peers = [row_peer(d) for d in range(1, ny)]
    cross_peers = [{**peer, **across} for across in row_peers for peer in col_peers + [{"gx": ix, "gz": iz}]]

    def spread(compact, slot):
        for t in range(ctiles):
            block = jnp.broadcast_to(compact[t:t + 1, :], (LANES, LANES))
            t_ref[slot, t * LANES:(t + 1) * LANES, :] = jnp.transpose(block)

    def squeeze(op):
        return jnp.concatenate(
            [op(jnp.transpose(t_ref[ga, t * LANES:(t + 1) * LANES, :]), axis=0, keepdims=True)
             for t in range(ctiles)], axis=0)

    factor = 2.0 * SCALE / width
    ones = jnp.ones((8, width), jnp.bfloat16)
    nt = (((1,), (1,)), ((), ()))
    group = math.gcd(CHUNK, 4)

    def fold(v, op):
        out = v[0:8]
        for q in range(1, v.shape[0] // 8):
            out = op(out, v[q * 8:(q + 1) * 8])
        return out

    def row_norm(v):
        square = v * v
        high = square.astype(jnp.bfloat16)
        low = (square - high.astype(F32)).astype(jnp.bfloat16)
        parts = [lax.dot_general(ones, part, nt, preferred_element_type=F32) for part in (high, low)]
        return (parts[0] + parts[1]) * (SCALE / width)

    y_copy.wait()
    x_copies[0].wait()
    yv = y_ref[...]
    yf = yv.astype(F32)
    ysq = row_norm(yf)
    kap = jnp.concatenate([ysq[0:1, t * LANES:(t + 1) * LANES] for t in range(ctiles)], axis=0)
    cap_ref[...] = kap
    spread(-kap, gb)

    def product(i):
        xb = x_ref[i * group * LANES:(i + 1) * group * LANES, :]
        prod = lax.dot_general(y_ref[...], xb, nt, preferred_element_type=F32)
        tops = [None] * group
        for s in range(nsub):
            sl = slice(s * SUB, (s + 1) * SUB)
            gv = t_ref[gb, sl, :]
            for q in range(group):
                val = prod[sl, q * LANES:(q + 1) * LANES] * factor + gv
                m_ref[i * group + q, sl, :] = val
                part = fold(val, jnp.maximum)
                tops[q] = part if tops[q] is None else jnp.maximum(tops[q], part)
        return [jnp.max(top, axis=0, keepdims=True) for top in tops]

    def row_sums(i, tops):
        tots = [None] * group
        for s in range(nsub):
            sl = slice(s * SUB, (s + 1) * SUB)
            for q in range(group):
                part = fold(jnp.exp2(m_ref[i * group + q, sl, :] - tops[q]), jnp.add)
                tots[q] = part if tots[q] is None else tots[q] + part
        c, at = divmod(i * group, CHUNK)
        for q in range(group):
            rbuf0[c, iy, at + q:at + q + 1, :] = tops[q]
            rbuf0[c, iy, CHUNK + at + q:CHUNK + at + q + 1, :] = jnp.sum(tots[q], axis=0, keepdims=True)

    steps = tiles // group
    per = CHUNK // group
    half = chunks // 2 * per
    tops = product(0)
    for i in range(steps):
        if i + 1 == half:
            x_copies[1].wait()
            for copy in m_copies:
                copy.wait()
            for c in range(chunks):
                rbuf0[c, iy, 2 * CHUNK:2 * CHUNK + 1, :] = jnp.sum(cm_ref[...], axis=0, keepdims=True)
                rbuf0[c, iy, 2 * CHUNK + 1:2 * CHUNK + 1 + ctiles, :] = cm_ref[...]
        ahead = product(i + 1) if i + 1 < steps else None
        row_sums(i, tops)
        tops = ahead
        if i + 1 == half:
            pl.semaphore_wait(barrier, ng * ny - 1)
            for c in range(half // per):
                send(rbuf0.at[c, iy], s_r0.at[c], r_r0.at[c], row_peers)
        elif i + 1 > half and (i + 1) % per == 0:
            c = i // per
            send(rbuf0.at[c, iy], s_r0.at[c], r_r0.at[c], row_peers)
    for c in range(chunks):
        drain(rbuf0.at[c, 0:ny - 1], r_r0.at[c])
        top = rbuf0[c, 0, 0:CHUNK, :]
        for d in range(1, ny):
            top = jnp.maximum(top, rbuf0[c, d, 0:CHUNK, :])
        tot = jnp.zeros((CHUNK, LANES), F32)
        for d in range(ny):
            tot = tot + rbuf0[c, d, CHUNK:2 * CHUNK, :] * jnp.exp2(rbuf0[c, d, 0:CHUNK, :] - top)
        lse = top + jnp.log2(tot)
        sl8 = slice(c * CHUNK, (c + 1) * CHUNK)
        lse_ref[sl8, :] = lse
        fv = jnp.log2(rm_ref[sl8, :]) - lse
        f_ref[sl8, :] = fv
        t_ref[gu, sl8, :] = fv
        for s in range(nsub):
            sl = slice(s * SUB, (s + 1) * SUB)
            acc = t_ref[ga, sl, :] if c else None
            for q in range(c * CHUNK, (c + 1) * CHUNK):
                val = m_ref[q, sl, :] + t_ref[gu, q:q + 1, :]
                t_ref[q, sl, :] = val
                acc = val if acc is None else jnp.maximum(acc, val)
            t_ref[ga, sl, :] = acc
    for c in range(chunks):
        drain(rbuf0.at[c, 0:ny - 1], s_r0.at[c])
    ctop = squeeze(jnp.max)
    spread(ctop, gb)
    for c in range(chunks):
        for s in range(nsub):
            sl = slice(s * SUB, (s + 1) * SUB)
            acc = t_ref[ga, sl, :] if c else None
            gv = t_ref[gb, sl, :]
            for q in range(c * CHUNK, (c + 1) * CHUNK):
                val = jnp.exp2(t_ref[q, sl, :] - gv)
                t_ref[q, sl, :] = val
                acc = val if acc is None else acc + val
            t_ref[ga, sl, :] = acc
    ctot = rbuf0[0, 0, 2 * CHUNK:2 * CHUNK + 1, :]
    for d in range(1, ny):
        ctot = ctot + rbuf0[0, d, 2 * CHUNK:2 * CHUNK + 1, :]
    mass = rm_ref[...]
    cbuf0[me, 0:ctiles, :] = ctop
    cbuf0[me, ctiles:2 * ctiles, :] = squeeze(jnp.sum)
    cbuf0[me, 2 * ctiles:2 * ctiles + 1, :] = jnp.sum(mass, axis=0, keepdims=True)
    send(cbuf0.at[me], s_c0, r_c0, col_peers)
    b_ref[...] = cm_ref[...] / jnp.sum(ctot, axis=1, keepdims=True)

    def norms(i, carry):
        xf = x_ref[pl.ds(pl.multiple_of(i * group * LANES, group * LANES), group * LANES), :].astype(F32)
        sq = row_norm(xf)
        for q in range(group):
            rho_ref[pl.ds(i * group + q, 1), :] = sq[0:1, q * LANES:(q + 1) * LANES]
        return carry

    lax.fori_loop(0, tiles // group, norms, 0)
    errs_ref[...] = jnp.zeros_like(errs_ref)
    ebuf[iy] = jnp.zeros(ebuf.shape[1:], F32)
    drain(cbuf0.at[0:ng - 1], r_c0)
    top = cbuf0[0, 0:ctiles, :]
    rtot = cbuf0[0, 2 * ctiles:2 * ctiles + 1, :]
    for d in range(1, ng):
        top = jnp.maximum(top, cbuf0[d, 0:ctiles, :])
        rtot = rtot + cbuf0[d, 2 * ctiles:2 * ctiles + 1, :]
    tot = jnp.zeros((ctiles, LANES), F32)
    for d in range(ng):
        tot = tot + cbuf0[d, ctiles:2 * ctiles, :] * jnp.exp2(cbuf0[d, 0:ctiles, :] - top)
    bv = b_ref[...]
    v_ref[...] = bv * jnp.exp2(cbuf0[me, 0:ctiles, :] - top) / tot
    rtot = jnp.sum(rtot, axis=1, keepdims=True)
    lrt = jnp.log2(rtot)
    a = rm_ref[...] / rtot
    a_ref[...] = a
    f_ref[...] = f_ref[...] - lrt
    err0_ref[...] = jnp.sum(jnp.abs(jnp.exp2(lse_ref[...] - rho_ref[...]) - a), axis=0, keepdims=True)
    clse = top + jnp.log2(tot) - lrt
    kap = cap_ref[...]
    gc_ref[...] = jnp.log2(bv) - clse - kap
    le_ref[...] = jnp.sum(jnp.abs(jnp.exp2(clse) - bv), axis=0, keepdims=True)
    drain(cbuf0.at[0:ng - 1], s_c0)

    def rebuild(i, carry):
        fvs = [f_ref[pl.ds(i * group + q, 1), :] for q in range(group)]
        for s in range(nsub):
            sl = slice(s * SUB, (s + 1) * SUB)
            gv = t_ref[gl, sl, :]
            for q in range(group):
                t_ref[i * group + q, sl, :] = jnp.exp2((m_ref[i * group + q, sl, :] + gv) + fvs[q])
        return carry

    def iteration(k, carry):
        par = lax.rem(k, 2)
        spread(v_ref[...], gb)
        for n, (lo, hi) in enumerate(pieces):
            tots = [None] * (hi - lo)
            for s in range(nsub):
                sl = slice(s * SUB, (s + 1) * SUB)
                gv = t_ref[gb, sl, :]
                for q in range(lo, hi):
                    part = fold(t_ref[q, sl, :] * gv, jnp.add)
                    tots[q - lo] = part if tots[q - lo] is None else tots[q - lo] + part
            for q in range(lo, hi):
                rbuf[par, iy, q:q + 1, :] = jnp.sum(tots[q - lo], axis=0, keepdims=True)
            send(rbuf.at[par, iy, lo:hi], s_r.at[par, n], r_r.at[par, n], row_peers)
        subs = LANES // SUB
        def receive(n):
            lo, hi = pieces[n]
            drain(rbuf.at[par, 0:ny - 1, lo:hi], r_r.at[par, n])
            r = rbuf[par, 0, lo:hi, :]
            for d in range(1, ny):
                r = r + rbuf[par, d, lo:hi, :]
            r_ref[lo:hi, :] = r
            t_ref[gu, lo:hi, :] = a_ref[lo:hi, :] / r

        receive(0)
        for n, (lo, hi) in enumerate(pieces):
            last = n == len(pieces) - 1
            for t in range(ctiles):
                if t == ctiles - 1 and not last:
                    receive(n + 1)
                block = []
                for s in range(t * subs, (t + 1) * subs):
                    sl = slice(s * SUB, (s + 1) * SUB)
                    acc = t_ref[ga, sl, :] if n else None
                    for q in range(lo, hi):
                        val = t_ref[q, sl, :] * t_ref[gu, q:q + 1, :]
                        acc = val if acc is None else acc + val
                    if not last:
                        t_ref[ga, sl, :] = acc
                    block.append(acc)
                if last:
                    line = jnp.sum(jnp.transpose(jnp.concatenate(block, axis=0)), axis=0, keepdims=True)
                    cbuf[par, me, t:t + 1, :] = line * v_ref[t:t + 1, :]
        cbuf[par, me, ctiles:ctiles + 1, :] = jnp.sum(jnp.abs(r_ref[...] - a_ref[...]), axis=0, keepdims=True)
        cbuf[par, me, ctiles + 1:ctiles + 2, :] = err0_ref[...]
        send(cbuf.at[par, me, 0:ctiles + 2], s_c.at[par], r_c.at[par], col_peers)
        ebuf[iy, pl.ds(k - 1, 1), :] = le_ref[...]

        @pl.when(k == ITERS - 1)
        def _():
            for peer in cross_peers:
                pltpu.make_async_remote_copy(
                    src_ref=cbuf.at[par, me, 0:ctiles], dst_ref=obuf.at[iy, me, 0:ctiles],
                    send_sem=s_o, recv_sem=r_o, device_id=peer, device_id_type=MESH).start()
            send(ebuf.at[iy], s_e, r_e, row_peers)

        f_ref[...] = f_ref[...] + jnp.log2(t_ref[gu, 0:tiles, :])
        spread(gc_ref[...] + cap_ref[...], gl)
        lax.fori_loop(0, tiles // group, rebuild, 0)
        for n, (lo, hi) in enumerate(pieces):
            drain(rbuf.at[par, 0:ny - 1, lo:hi], s_r.at[par, n])
        drain(cbuf.at[par, 0:ng - 1, 0:ctiles + 2], r_c.at[par])
        got = cbuf[par, 0]
        for d in range(1, ng):
            got = got + cbuf[par, d]
        old = got[0:ctiles]
        bv = b_ref[...]
        v = bv / old
        v_ref[...] = v
        gc_ref[...] = gc_ref[...] + jnp.log2(v)
        le_ref[...] = jnp.sum(jnp.abs(old - bv), axis=0, keepdims=True)
        errs_ref[pl.ds(k, 1), :] = got[ctiles:ctiles + 1]
        errs_ref[0:1, :] = got[ctiles + 1:ctiles + 2]
        drain(cbuf.at[par, 0:ng - 1, 0:ctiles + 2], s_c.at[par])
        return carry

    lax.fori_loop(1, ITERS, iteration, 0)
    f_out[...] = (f_ref[...] + rho_ref[...]) * (1.0 / SCALE)
    g_out[...] = (gc_ref[...] + cap_ref[...]) * (1.0 / SCALE)
    drain(ebuf.at[0:ny - 1], r_e)
    drain(ebuf.at[0:ny - 1], s_e)
    drain(obuf.at[0:ny - 1, 0:ng, 0:ctiles], r_o)
    ce = ebuf[0]
    for d in range(1, ny):
        ce = ce + ebuf[d]
    errs_ref[pad:2 * pad, :] = ce
    tail = le_ref[...]
    for d in range(1, ny):
        other = lax.rem(iy + d, ny)
        seen = obuf[other, 0, 0:ctiles, :]
        for c in range(1, ng):
            seen = seen + obuf[other, c, 0:ctiles, :]
        bo = rbuf0[0, other, 2 * CHUNK + 1:2 * CHUNK + 1 + ctiles, :] / jnp.sum(ctot, axis=1, keepdims=True)
        tail = tail + jnp.sum(jnp.abs(seen - bo), axis=0, keepdims=True)
    errs_ref[pad + ITERS - 1:pad + ITERS, :] = tail
    drain(obuf.at[0:ny - 1, 0:ng, 0:ctiles], s_o)
    both = jnp.sum(jnp.transpose(errs_ref[...]), axis=0, keepdims=True)
    e_out[0:1, :] = both[:, 0:ITERS]
    e_out[1:2, :] = both[:, pad:pad + ITERS]


def hand_on(f, g, e, f_out, g_out, e_out, sem):
    copies = [pltpu.make_async_copy(src, dst, sem.at[n])
              for n, (src, dst) in enumerate(((f, f_out), (g, g_out), (e, e_out)))]
    for copy in copies:
        copy.start()
    for copy in copies:
        copy.wait()


def on_device(row_embed, col_embed, row_mass, col_mass):
    rows, width = row_embed.shape
    cols = col_embed.shape[0]
    nx, nz, ny = lax.axis_size("gx"), lax.axis_size("gz"), lax.axis_size("gy")
    ng = nx * nz
    tiles, ctiles = rows // LANES, cols // LANES
    chunks = tiles // CHUNK
    npieces = len(row_pieces(tiles))
    pad = -(-ITERS // 8) * 8
    crow0 = -(-(2 * ctiles + 1) // 8) * 8
    crow = -(-(ctiles + 2) // 8) * 8
    vm = lambda *s: pltpu.VMEM(s, F32)
    dma = pltpu.SemaphoreType.DMA
    f, g, e = pl.pallas_call(
        functools.partial(kernel, nx, nz, ny),
        out_shape=(jax.ShapeDtypeStruct((tiles, LANES), F32),
                   jax.ShapeDtypeStruct((ctiles, LANES), F32),
                   jax.ShapeDtypeStruct((2, ITERS), F32)),
        in_specs=[pl.BlockSpec(memory_space=pl.ANY)] * 4,
        out_specs=[pl.BlockSpec(memory_space=pltpu.VMEM)] * 3,
        scratch_shapes=[
            vm(tiles, cols, LANES), vm(tiles + 4, cols, LANES),
            vm(tiles, LANES), vm(tiles, LANES), vm(tiles, LANES), vm(tiles, LANES),
            vm(ctiles, LANES), vm(ctiles, LANES), vm(ctiles, LANES),
            vm(1, LANES), vm(1, LANES), vm(LANES, LANES), vm(CHUNK, LANES), vm(ctiles, LANES),
            vm(tiles, LANES), vm(chunks, ny, 3 * CHUNK, LANES), vm(2, ny, tiles, LANES),
            vm(ng, crow0, LANES), vm(2, ng, crow, LANES), vm(ny, pad, LANES), vm(ny, ng, ctiles, LANES),
            pltpu.VMEM((rows, width), row_embed.dtype), pltpu.VMEM((cols, width), col_embed.dtype),
            vm(tiles, LANES), vm(ctiles, LANES), dma((2,)), dma, dma((2,)), dma((chunks,)), dma((chunks,)), dma((2, npieces)), dma((2, npieces)), dma, dma, dma((2,)), dma((2,)), dma, dma, dma, dma,
        ],
        compiler_params=pltpu.CompilerParams(
            collective_id=0, has_side_effects=True, vmem_limit_bytes=67043328),
    )(row_embed, col_embed, row_mass.reshape(tiles, LANES), col_mass.reshape(ctiles, LANES))
    f, g, e = pl.pallas_call(
        hand_on,
        out_shape=tuple(jax.ShapeDtypeStruct(v.shape, F32) for v in (f, g, e)),
        in_specs=[pl.BlockSpec(memory_space=pl.ANY)] * 3,
        out_specs=[pl.BlockSpec(memory_space=pl.ANY)] * 3,
        scratch_shapes=[dma((3,))],
    )(f, g, e)
    return f.reshape(rows), g.reshape(cols), e.T


def solution(mesh):
    in_specs = (P(("gx", "gz"), None), P("gy", None), P(("gx", "gz")), P("gy"))
    out_specs = (P(("gx", "gz")), P("gy"), P())
    return jax.shard_map(
        on_device, mesh=mesh, in_specs=in_specs, out_specs=out_specs, check_vma=False
    )
```
